256 devices in a mesh: dp: 4 (over y), space: 64 (over x, z, core).
Axes of the slice: x: 4, y: 4, z: 8, core: 2. Of those that a mesh axis runs over, the one named last changes fastest.
Arguments:
- queries: bfloat16 [32, 200, 256], P('dp'), may hold values from -6 to 6
- query_pos: bfloat16 [200, 256], replicated, may hold values from -6 to 6
- pixels: bfloat16 [32, 16384, 256], P('dp', 'space'), may hold values from -160 to 160
- pixel_pos: bfloat16 [16384, 256], P('space'), may hold values from -6 to 6
- masks: int32 [32, 200, 16384], P('dp', None, 'space'), may hold values from 0 to 1, as said below
- wq_cross: bfloat16 [256, 256], replicated, may hold values from -0.375 to 0.375
- wk_cross: bfloat16 [256, 256], replicated, may hold values from -0.375 to 0.375
- wv_cross: bfloat16 [256, 256], replicated, may hold values from -0.375 to 0.375
- wo_cross: bfloat16 [256, 256], replicated, may hold values from -0.375 to 0.375
- gain_cross: float32 [256], replicated, may hold values from 0.1 to 1.9
- w_qkv: bfloat16 [256, 768], replicated, may hold values from -0.375 to 0.375
- wo_self: bfloat16 [256, 256], replicated, may hold values from -0.375 to 0.375
- gain_self: float32 [256], replicated, may hold values from 0.1 to 1.9
- w_in: bfloat16 [256, 2048], replicated, may hold values from -0.375 to 0.375
- w_out: bfloat16 [2048, 256], replicated, may hold values from -0.125 to 0.125
- gain_ffn: float32 [256], replicated, may hold values from 0.1 to 1.9
Outputs:
- new_queries: bfloat16 [32, 200, 256], P('dp')
The draws below stay inside these ranges and needn't reach their ends.
Inputs may be any that keep to these rules, and one draw needn't show every extreme that they name: `masks`: 0 or 1; each row's ones lie within a run of at most 768 consecutive pixels, which may lie anywhere in the image; a row may have no ones on some devices' pixels or on all pixels of its image.
All inputs are finite; a program needn't handle non-finite values.
Results may differ from the reference program's by a relative error of at most 0.017.
The reference program's roundings to bfloat16 on the way (of `query_in`, `cross_q`, `attended`, `after_cross`, `self_weight`, `self_out`, `after_self` and `hidden`) count: a program that leaves them out, or rounds other values in their place, can miss the bound.
Values may be sent and summed in bfloat16 or wider, within the bound.
A program may use at most 128 MiB of HBM per device.

```python
import jax
import jax.numpy as jnp
from jax import lax

D = 256
HEADS = 8
Q = 200
FF = 2048
IMG_DP = 8
PIX_DEV = 256
IMAGES = 32
PIXELS = 16384


def draw_masks(key, part):
    k_span, k_full, k_start, k_heavy, k_rate, k_empty, k_bits, k_anchor = jax.random.split(jax.random.fold_in(key, 11), 8)
    longest = 3 * PIX_DEV
    spread = PIXELS // PIX_DEV
    row_ids = jnp.arange(Q, dtype=jnp.int32)[None, :, None]
    image_ids = jnp.arange(IMAGES, dtype=jnp.int32)[:, None, None]
    span = jax.random.randint(k_span, (IMAGES, Q, 1), 1, longest + 1)
    full_row = jax.random.randint(k_full, (IMAGES, 1, 1), 0, Q)
    is_full = row_ids == full_row
    span = jnp.where(is_full, longest, span)
    start = jax.random.randint(k_start, (IMAGES, Q, 1), 0, PIXELS - span + 1)
    share = (IMG_DP * Q + spread - 1) // spread
    group_row = image_ids % IMG_DP * Q + row_ids
    far_dev = (group_row // share + spread // 2) % spread
    anchored = jax.random.randint(k_anchor, (IMAGES, Q, 1), 0, 4) == 0
    far_start = jnp.minimum(far_dev * PIX_DEV, PIXELS - span)
    start = jnp.where(anchored, far_start, start)
    heavy_pick = jax.random.randint(k_heavy, (), 0, min(4, IMAGES))
    heavy = image_ids % 4 == heavy_pick
    rate = jnp.where(heavy, 31, jax.random.randint(k_rate, (IMAGES, 1, 1), 0, 33))
    empty = (jax.random.randint(k_empty, (IMAGES, Q, 1), 0, 32) < rate) & jnp.logical_not(is_full) & jnp.logical_not(anchored)
    where_at = jnp.arange(PIXELS, dtype=jnp.int32)[None, None, :]
    ends = (where_at == start) | (where_at == start + span - 1)
    inside = (where_at >= start) & (where_at < start + span)
    bits = (jax.random.randint(k_bits, (IMAGES, Q, PIXELS), 0, 4) > 0) | ends
    keep = inside & bits & jnp.logical_not(empty)
    return keep.astype(jnp.int32)


def draw_pixels(key, part):
    k_base = jax.random.fold_in(jax.random.fold_in(key, 23), 0)
    base = jnp.clip(jax.random.normal(k_base, (IMAGES, PIXELS, D), jnp.float32), -4.0, 4.0)
    return base.astype(jnp.bfloat16)


def shard_levels(stream_key, dims, cuts, low, top_value):
    def one(position, blocks):
        heights = jax.random.uniform(jax.random.fold_in(jax.random.fold_in(stream_key, 6), position), (blocks,), jnp.float32, low / len(cuts), top_value / len(cuts))
        return jnp.repeat(jnp.exp(heights), dims[position] // blocks).reshape((-1,) + (1,) * (len(dims) - position - 1))

    loudness = one(*cuts[0])
    for cut in cuts[1:]:
        loudness = loudness * one(*cut)
    return loudness


def noise(own_key, shape, deviation, reach, shards=(), kind=jnp.bfloat16):
    level = shard_levels(own_key, shape, shards, -0.22, 0.18) if shards else 1.0
    values = jax.random.normal(own_key, shape, jnp.float32) * deviation * level
    return jnp.minimum(jnp.maximum(values, -reach), reach).astype(kind)


def setup_inputs(seed: int = 0) -> dict:
    arg_keys = jax.random.split(jax.random.key(seed), 17)
    return {
        "queries": noise(arg_keys[0], (IMAGES, Q, D), 1.0, 6.0, ((0, 4),)),
        "query_pos": noise(arg_keys[1], (Q, D), 1.0, 6.0),
        "pixels": draw_pixels(jax.random.fold_in(arg_keys[16], 71), 0),
        "pixel_pos": noise(arg_keys[3], (PIXELS, D), 1.0, 6.0, ((0, 64),)),
        "masks": draw_masks(jax.random.fold_in(arg_keys[16], 71), 0),
        "wq_cross": noise(arg_keys[5], (D, D), D ** -0.5, 0.375),
        "wk_cross": noise(arg_keys[6], (D, D), D ** -0.5, 0.375),
        "wv_cross": noise(arg_keys[7], (D, D), D ** -0.5, 0.375),
        "wo_cross": noise(arg_keys[8], (D, D), D ** -0.5, 0.375),
        "gain_cross": jnp.clip(1.0 + 0.18 * jax.random.normal(arg_keys[9], (D,), jnp.float32), 0.1, 1.9),
        "w_qkv": noise(arg_keys[10], (D, 3 * D), D ** -0.5, 0.375),
        "wo_self": noise(arg_keys[11], (D, D), D ** -0.5, 0.375),
        "gain_self": jnp.clip(1.0 + 0.18 * jax.random.normal(arg_keys[12], (D,), jnp.float32), 0.1, 1.9),
        "w_in": noise(arg_keys[13], (D, FF), D ** -0.5, 0.375),
        "w_out": noise(arg_keys[14], (FF, D), FF ** -0.5, 0.125),
        "gain_ffn": jnp.clip(1.0 + 0.18 * jax.random.normal(arg_keys[15], (D,), jnp.float32), 0.1, 1.9),
    }


def layer_norm(x, gain):
    mean = lax.optimization_barrier(jnp.mean(x, axis=-1, keepdims=True))
    var = lax.optimization_barrier(jnp.mean((x - mean) * (x - mean), axis=-1, keepdims=True))
    return (x - mean) / jnp.sqrt(var + 1e-05) * gain

def decoder_rest(queries, attended, query_pos, wo_cross, gain_cross, w_qkv, wo_self, gain_self, w_in, w_out, gain_ffn):
    images, nq, width = queries.shape
    heads = HEADS
    head_size = width // heads
    flat_att = attended.reshape(images * nq, width)
    cross_proj = jnp.dot(flat_att, wo_cross, preferred_element_type=jnp.float32)
    flat_q = queries.reshape(images * nq, width).astype(jnp.float32)
    after_cross = layer_norm(flat_q + cross_proj, gain_cross).astype(jnp.bfloat16)
    pos_rows = jnp.tile(query_pos.astype(jnp.float32), (images, 1))
    self_in = (after_cross.astype(jnp.float32) + pos_rows).astype(jnp.bfloat16)
    both = jnp.dot(self_in, w_qkv[:, :2 * width], preferred_element_type=jnp.float32).astype(jnp.bfloat16)
    self_v = jnp.dot(after_cross, w_qkv[:, 2 * width:], preferred_element_type=jnp.float32).astype(jnp.bfloat16)
    self_q = both[:, :width].reshape(images, nq, heads, head_size)
    self_k = both[:, width:].reshape(images, nq, heads, head_size)
    self_v = self_v.reshape(images, nq, heads, head_size)
    logits = jnp.einsum('iqhd,ikhd->ihqk', self_q.astype(jnp.float32), self_k.astype(jnp.float32)) / jnp.sqrt(jnp.float32(head_size))
    top = lax.optimization_barrier(jnp.max(logits, axis=-1, keepdims=True))
    expo = jnp.exp(logits - top)
    self_weight = (expo / lax.optimization_barrier(jnp.sum(expo, axis=-1, keepdims=True))).astype(jnp.bfloat16)
    self_out = jnp.einsum('ihqk,ikhd->iqhd', self_weight.astype(jnp.float32), self_v.astype(jnp.float32))
    self_out = self_out.astype(jnp.bfloat16).reshape(images * nq, width)
    self_proj = jnp.dot(self_out, wo_self, preferred_element_type=jnp.float32)
    after_self = layer_norm(after_cross.astype(jnp.float32) + self_proj, gain_self).astype(jnp.bfloat16)
    hidden = jnp.maximum(jnp.dot(after_self, w_in, preferred_element_type=jnp.float32), 0.0).astype(jnp.bfloat16)
    ffn_out = jnp.dot(hidden, w_out, preferred_element_type=jnp.float32)
    result = layer_norm(after_self.astype(jnp.float32) + ffn_out, gain_ffn).astype(jnp.bfloat16)
    return result.reshape(images, nq, width)

def reference(queries, query_pos, pixels, pixel_pos, masks, wq_cross, wk_cross, wv_cross, wo_cross, gain_cross, w_qkv, wo_self, gain_self, w_in, w_out, gain_ffn):
    head_size = D // HEADS
    query_in = (queries.astype(jnp.float32) + query_pos.astype(jnp.float32)[None]).astype(jnp.bfloat16)

    def one_image(items):
        qin, pix, mask = items
        cross_q = jnp.dot(qin, wq_cross, preferred_element_type=jnp.float32).astype(jnp.bfloat16).reshape(Q, HEADS, head_size)
        key_in = (pix.astype(jnp.float32) + pixel_pos.astype(jnp.float32)).astype(jnp.bfloat16)
        cross_k = jnp.dot(key_in, wk_cross, preferred_element_type=jnp.float32).astype(jnp.bfloat16).reshape(PIXELS, HEADS, head_size)
        cross_v = jnp.dot(pix, wv_cross, preferred_element_type=jnp.float32).astype(jnp.bfloat16).reshape(PIXELS, HEADS, head_size)
        count = lax.optimization_barrier(jnp.sum(mask, axis=-1))
        allowed = (mask > 0) | (count == 0)[:, None]
        score = jnp.einsum('qhd,phd->qhp', cross_q.astype(jnp.float32), cross_k.astype(jnp.float32)) / jnp.sqrt(jnp.float32(head_size))
        score = jnp.where(allowed[:, None, :], score, -jnp.inf)
        top = lax.optimization_barrier(jnp.max(score, axis=-1, keepdims=True))
        weight = jnp.where(allowed[:, None, :], jnp.exp(score - top), 0.0)
        total = lax.optimization_barrier(jnp.sum(weight, axis=-1))
        summed = jnp.einsum('qhp,phd->qhd', weight.astype(jnp.bfloat16).astype(jnp.float32), cross_v.astype(jnp.float32))
        return (summed / total[..., None]).astype(jnp.bfloat16).reshape(Q, D)
    attended = lax.map(one_image, (query_in, pixels, masks))
    return decoder_rest(queries, attended, query_pos, wo_cross, gain_cross, w_qkv, wo_self, gain_self, w_in, w_out, gain_ffn)
```

```python
import math

import jax
import jax.numpy as jnp
from jax import lax
from jax.experimental import pallas as pl
from jax.experimental.pallas import tpu as pltpu
from jax.sharding import PartitionSpec as P

HEADS = 8
HEAD = 32
NX = 4
NZ = 8
LANES = 256
FAR = -1e30
MESH = pl.DeviceIdType.MESH
F32 = jnp.float32
BF16 = jnp.bfloat16


def dot(a, b, contract=((1,), (0,))):
    return lax.dot_general(a, b, (contract, ((), ())), preferred_element_type=F32)


def dot_nt(a, b):
    return dot(a, b, ((1,), (1,)))


def layer_norm(x, gain):
    mean = jnp.mean(x, axis=-1, keepdims=True)
    d = x - mean
    var = jnp.mean(d * d, axis=-1, keepdims=True)
    return d / jnp.sqrt(var + 1e-05) * gain


def merge(tops, totals):
    most = totals[0]
    for t in totals[1:]:
        most = jnp.maximum(most, t)
    some = most > 0
    seen = [jnp.where(some & (t < 0), -3e38, m) for m, t in zip(tops, totals)]
    top = seen[0]
    for m in seen[1:]:
        top = jnp.maximum(top, m)
    scales = [jnp.exp2(m - top) for m in seen]
    total = scales[0] * jnp.abs(totals[0])
    for s, t in zip(scales[1:], totals[1:]):
        total = total + s * jnp.abs(t)
    return top, jnp.where(some, total, -total), scales


def kernel(
    queries, query_pos, pixels, pixel_pos, masks, wq, wk, wv, wo, gain_cross, w_qkv, wo_self, gain_self, w_in, w_out,
    gain_ffn,
    out,
    wq_t, wv_t, eye, keys, values_t, query_t, bias, own_o, own_m,
    p1o, p1m, r1o, r1m, p2o, p2m, r2o, r2m, p3o, p3m, r3o, r3m, att,
    s1, v1, s2, v2, s3, v3, s4, v4, s5, v5, s6, v6,
):
    nq = queries.shape[1]
    width = queries.shape[2]
    pix = pixels.shape[1]
    me = lax.axis_index("space")
    core = lax.rem(me, 2)
    z = lax.rem(me // 2, NZ)
    x = me // (2 * NZ)
    factor = math.log2(math.e) / math.sqrt(HEAD)

    def at(xx, zz, cc):
        return {"space": (xx * NZ + zz) * 2 + cc}

    def x_peer(d):
        return at(lax.rem(x + d, NX), z, core)

    def z_peer(d):
        return at(x, lax.rem(z + d, NZ), core)

    partner = at(x, z, 1 - core)

    barrier = pltpu.get_barrier_semaphore()
    pl.semaphore_signal(barrier, inc=1, device_id=partner, device_id_type=MESH)
    for d in range(1, NX):
        pl.semaphore_signal(barrier, inc=1, device_id=x_peer(d), device_id_type=MESH)
    for d in range(1, NZ):
        pl.semaphore_signal(barrier, inc=1, device_id=z_peer(d), device_id_type=MESH)

    def send(src, dst, send_sem, recv_sem, where):
        return pltpu.make_async_remote_copy(
            src_ref=src, dst_ref=dst, send_sem=send_sem, recv_sem=recv_sem, device_id=where, device_id_type=MESH
        )

    rows = lax.broadcasted_iota(jnp.int32, (pix, pix), 0)
    cols = lax.broadcasted_iota(jnp.int32, (pix, pix), 1)
    eye[...] = jnp.where(rows == cols, 1.0, 0.0).astype(BF16)
    wq_t[...] = dot_nt(eye[...], wq[...]).astype(BF16)
    wv_t[...] = dot_nt(eye[...], wv[...]).astype(BF16)
    query_t[...] = jnp.zeros_like(query_t)
    bias[...] = jnp.zeros_like(bias)
    for h in range(HEADS):
        values_t[h, HEAD:, :] = jnp.ones((16, pix), BF16)

    def partial(i, put_o, m_ref):
        one = pixels[i]
        key_in = (one.astype(F32) + pixel_pos[...].astype(F32)).astype(BF16)
        keys[...] = dot(key_in, wk[...]).astype(BF16)
        v_t = dot_nt(wv_t[...], one).astype(BF16)
        for h in range(HEADS):
            values_t[h, :HEAD, :] = v_t[h * HEAD : (h + 1) * HEAD, :]
        query_in = (queries[i].astype(F32) + query_pos[...].astype(F32)).astype(BF16)
        query_t[:, :nq] = dot_nt(wq_t[...], query_in).astype(BF16)
        mask_t = dot_nt(eye[...], masks[i].astype(F32).astype(BF16))
        count = jnp.sum(mask_t, axis=0, keepdims=True)
        bias[:, :nq] = jnp.where((mask_t > 0.5) | (count == 0.0), 0.0, FAR)
        sign = jnp.where(count == 0.0, -1.0, 1.0)
        for h in range(HEADS):
            tile = (h // 4) * 128
            lane = (h % 4) * HEAD
            parts = []
            if lane:
                parts.append(jnp.zeros((lane, LANES), BF16))
            parts.append(query_t[h * HEAD : (h + 1) * HEAD, :])
            if lane + HEAD < 128:
                parts.append(jnp.zeros((128 - lane - HEAD, LANES), BF16))
            one_head = jnp.concatenate(parts, axis=0)
            score = dot(keys[:, tile : tile + 128], one_head) * factor + bias[...]
            top = jnp.max(score, axis=0, keepdims=True)
            weight = jnp.exp2(score - top).astype(BF16)
            both = dot(values_t[h], weight)
            put_o(h, both[:HEAD])
            m_ref[h : h + 1, :] = top
            m_ref[HEADS + h : HEADS + h + 1, :] = both[HEAD : HEAD + 1]
        m_ref[HEADS:, :nq] = m_ref[HEADS:, :nq] * sign

    def first(j, carry):
        i = (1 - core) * NX + lax.rem(x + j + 1, NX)

        def put(h, value):
            p1o[j, h * HEAD : (h + 1) * HEAD, :] = value.astype(BF16)

        partial(i, put, p1m.at[j])

        @pl.when(j == 0)
        def _():
            pl.semaphore_wait(barrier, NX + NZ - 1)

        send(p1o.at[j], r1o.at[j], s1.at[j, 0], v1.at[j, 0], partner).start()
        send(p1m.at[j], r1m.at[j], s1.at[j, 1], v1.at[j, 1], partner).start()
        return carry

    lax.fori_loop(0, NX, first, 0)

    def second(j, carry):
        i = core * NX + lax.rem(x + j + 1, NX)

        def put(h, value):
            own_o[h * HEAD : (h + 1) * HEAD, :] = value

        partial(i, put, own_m)
        a = send(p1o.at[j], r1o.at[j], s1.at[j, 0], v1.at[j, 0], partner)
        b = send(p1m.at[j], r1m.at[j], s1.at[j, 1], v1.at[j, 1], partner)
        a.wait()
        b.wait()
        top, total, scales = merge([own_m[:HEADS], r1m[j, :HEADS]], [own_m[HEADS:], r1m[j, HEADS:]])
        p2m[j, :HEADS] = top
        p2m[j, HEADS:] = total
        for h in range(HEADS):
            part = slice(h * HEAD, (h + 1) * HEAD)
            folded = own_o[part] * scales[0][h : h + 1] + r1o[j, part].astype(F32) * scales[1][h : h + 1]
            p2o[j, part] = folded.astype(BF16)

        @pl.when(j < NX - 1)
        def _():
            to = x_peer(j + 1)
            send(p2o.at[j], r2o.at[j], s2.at[j, 0], v2.at[j, 0], to).start()
            send(p2m.at[j], r2m.at[j], s2.at[j, 1], v2.at[j, 1], to).start()

        return carry

    lax.fori_loop(0, NX, second, 0)

    mine = NX - 1
    for j in range(NX - 1):
        to = x_peer(j + 1)
        send(p2o.at[j], r2o.at[j], s2.at[j, 0], v2.at[j, 0], to).wait()
        send(p2m.at[j], r2m.at[j], s2.at[j, 1], v2.at[j, 1], to).wait()
    tops = [p2m[mine, :HEADS]] + [r2m[j, :HEADS] for j in range(NX - 1)]
    totals = [p2m[mine, HEADS:]] + [r2m[j, HEADS:] for j in range(NX - 1)]
    top, total, scales = merge(tops, totals)
    for h in range(HEADS):
        part = slice(h * HEAD, (h + 1) * HEAD)
        folded = p2o[mine, part].astype(F32) * scales[0][h : h + 1]
        for j in range(NX - 1):
            folded = folded + r2o[j, part].astype(F32) * scales[j + 1][h : h + 1]
        p3o[h] = folded.astype(BF16)
        p3m[h, 0:1] = top[h : h + 1]
        p3m[h, 1:2] = total[h : h + 1]

    def z_send(d):
        h = lax.rem(z + d, NZ)
        return (
            send(p3o.at[h], r3o.at[d - 1], s3.at[d - 1, 0], v3.at[d - 1, 0], z_peer(d)),
            send(p3m.at[h], r3m.at[d - 1], s3.at[d - 1, 1], v3.at[d - 1, 1], z_peer(d)),
        )

    order = (4, 3, 5, 2, 6, 1, 7)
    for d in order:
        for copy in z_send(d):
            copy.start()
    for d in order[::-1]:
        for copy in z_send(d):
            copy.wait()
    tops = [p3m[z, 0:1]] + [r3m[d, 0:1] for d in range(NZ - 1)]
    totals = [p3m[z, 1:2]] + [r3m[d, 1:2] for d in range(NZ - 1)]
    top, total, scales = merge(tops, totals)
    folded = p3o[z].astype(F32) * scales[0]
    for d in range(NZ - 1):
        folded = folded + r3o[d].astype(F32) * scales[d + 1]
    att[z] = (folded / jnp.abs(total)).astype(BF16)

    def z_gather(d):
        return send(att.at[z], att.at[z], s4.at[d - 1], v4.at[d - 1], z_peer(d))

    for d in order:
        z_gather(d).start()
    for d in order[::-1]:
        z_gather(d).wait()

    i_own = core * NX + x
    attended_t = att[...].reshape(width, LANES)
    cross = dot(attended_t, wo[...], ((0,), (0,)))[:nq]
    pos = query_pos[...].astype(F32)
    after_cross = layer_norm(queries[i_own].astype(F32) + cross, gain_cross[...]).astype(BF16)
    self_in = (after_cross.astype(F32) + pos).astype(BF16)
    both = dot(self_in, w_qkv[:, : 2 * width]).astype(BF16)
    self_v = dot(after_cross, w_qkv[:, 2 * width :]).astype(BF16)
    head_of = lax.broadcasted_iota(jnp.int32, (nq, 128), 1) // HEAD
    outs = []
    for tile in range(width // 128):
        part = slice(tile * 128, (tile + 1) * 128)
        q_tile = both[:, part].astype(F32)
        k_tile = both[:, width + tile * 128 : width + (tile + 1) * 128]
        v_tile = self_v[:, part]
        gathered = jnp.zeros((nq, 128), F32)
        for h in range(128 // HEAD):
            q_head = jnp.where(head_of == h, q_tile, 0.0).astype(BF16)
            logits = dot_nt(q_head, k_tile) * (1.0 / math.sqrt(HEAD))
            top = jnp.max(logits, axis=-1, keepdims=True)
            expo = jnp.exp(logits - top)
            weight = (expo / jnp.sum(expo, axis=-1, keepdims=True)).astype(BF16)
            gathered = jnp.where(head_of == h, dot(weight, v_tile), gathered)
        outs.append(gathered.astype(BF16))
    self_proj = dot(jnp.concatenate(outs, axis=1), wo_self[...])
    after_self = layer_norm(after_cross.astype(F32) + self_proj, gain_self[...]).astype(BF16)
    hidden = jnp.maximum(dot(after_self, w_in[...]), 0.0).astype(BF16)
    ffn = dot(hidden, w_out[...])
    out[i_own] = layer_norm(after_self.astype(F32) + ffn, gain_ffn[...]).astype(BF16)

    def x_out(d):
        return send(out.at[i_own], out.at[i_own], s5.at[d - 1], v5.at[d - 1], x_peer(d))

    def core_out(k):
        i = core * NX + lax.rem(x - k + NX, NX)
        return send(out.at[i], out.at[i], s6.at[k], v6.at[k], partner)

    for d in (2, 1, 3):
        x_out(d).start()
    core_out(0).start()
    for d in (1, 3, 2):
        x_out(d).wait_recv()
        core_out(d).start()
    for d in (1, 2, 3):
        x_out(d).wait_send()
    for k in range(NX):
        core_out(k).wait()


def local(
    queries, query_pos, pixels, pixel_pos, masks, wq_cross, wk_cross, wv_cross, wo_cross, gain_cross, w_qkv, wo_self,
    gain_self, w_in, w_out, gain_ffn,
):
    images, nq, width = queries.shape
    pix = pixels.shape[1]
    dma = pltpu.SemaphoreType.DMA
    vmem = pltpu.VMEM
    scratch = [
        vmem((width, width), BF16),
        vmem((width, width), BF16),
        vmem((pix, pix), BF16),
        vmem((pix, width), BF16),
        vmem((HEADS, HEAD + 16, pix), BF16),
        vmem((width, LANES), BF16),
        vmem((pix, LANES), F32),
        vmem((width, LANES), F32),
        vmem((2 * HEADS, LANES), F32),
        vmem((NX, width, LANES), BF16),
        vmem((NX, 2 * HEADS, LANES), F32),
        vmem((NX, width, LANES), BF16),
        vmem((NX, 2 * HEADS, LANES), F32),
        vmem((NX, width, LANES), BF16),
        vmem((NX, 2 * HEADS, LANES), F32),
        vmem((NX - 1, width, LANES), BF16),
        vmem((NX - 1, 2 * HEADS, LANES), F32),
        vmem((NZ, HEAD, LANES), BF16),
        vmem((NZ, 8, LANES), F32),
        vmem((NZ - 1, HEAD, LANES), BF16),
        vmem((NZ - 1, 8, LANES), F32),
        vmem((NZ, HEAD, LANES), BF16),
        dma((NX, 2)),
        dma((NX, 2)),
        dma((NX - 1, 2)),
        dma((NX - 1, 2)),
        dma((NZ - 1, 2)),
        dma((NZ - 1, 2)),
        dma((NZ - 1,)),
        dma((NZ - 1,)),
        dma((NX - 1,)),
        dma((NX - 1,)),
        dma((NX,)),
        dma((NX,)),
    ]
    return pl.pallas_call(
        kernel,
        out_shape=jax.ShapeDtypeStruct((images, nq, width), BF16),
        in_specs=[pl.BlockSpec(memory_space=pltpu.VMEM)] * 16,
        out_specs=pl.BlockSpec(memory_space=pltpu.VMEM),
        scratch_shapes=scratch,
        compiler_params=pltpu.CompilerParams(
            collective_id=0, has_side_effects=True, vmem_limit_bytes=48 * 1024 * 1024
        ),
        name="decoder_layer",
    )(
        queries, query_pos, pixels, pixel_pos, masks, wq_cross, wk_cross, wv_cross, wo_cross, gain_cross[None], w_qkv,
        wo_self, gain_self[None], w_in, w_out, gain_ffn[None],
    )


def solution(mesh):
    placed = (
        P("dp", None, None),
        P(),
        P("dp", "space", None),
        P("space", None),
        P("dp", None, "space"),
    ) + (P(),) * 11
    return jax.shard_map(local, mesh=mesh, in_specs=placed, out_specs=P("dp", None, None), check_vma=False)
```

```python
import math

import jax
import jax.numpy as jnp
from jax import lax
from jax.experimental import pallas as pl
from jax.experimental.pallas import tpu as pltpu
from jax.sharding import PartitionSpec as P

HEADS = 8
HEAD = 32
NX = 4
NZ = 8
LANES = 256
FAR = -1e30
MESH = pl.DeviceIdType.MESH
F32 = jnp.float32
BF16 = jnp.bfloat16


def dot(a, b, contract=((1,), (0,))):
    return lax.dot_general(a, b, (contract, ((), ())), preferred_element_type=F32)


def dot_nt(a, b):
    return dot(a, b, ((1,), (1,)))


def layer_norm(x, gain):
    mean = jnp.mean(x, axis=-1, keepdims=True)
    d = x - mean
    var = jnp.mean(d * d, axis=-1, keepdims=True)
    return d / jnp.sqrt(var + 1e-05) * gain


def merge(tops, totals):
    most = totals[0]
    for t in totals[1:]:
        most = jnp.maximum(most, t)
    some = most > 0
    seen = [jnp.where(some & (t < 0), -3e38, m) for m, t in zip(tops, totals)]
    top = seen[0]
    for m in seen[1:]:
        top = jnp.maximum(top, m)
    scales = [jnp.exp2(m - top) for m in seen]
    total = scales[0] * jnp.abs(totals[0])
    for s, t in zip(scales[1:], totals[1:]):
        total = total + s * jnp.abs(t)
    return top, jnp.where(some, total, -total), scales


def kernel(
    queries_in, query_pos_in, pixels_in, pixel_pos_in, masks_in, wq_in, wk_in, wv_in, wo_in, gain_cross_in, w_qkv_in,
    wo_self_in, gain_self_in, w_in_in, w_out_in, gain_ffn_in,
    out,
    queries, query_pos, pixels, pixel_pos, masks, wq, wk, wv, wo, gain_cross, w_qkv, wo_self, gain_self, w_in, w_out,
    gain_ffn, image_sem, early_sem, late_sem,
    wq_t, wv_t, eye, keys, values_t, query_t, bias, scores, weights, own_o, own_m,
    p1o, p1m, r1o, r1m, p2o, p2m, r2o, r2m, p3o, p3m, r3o, r3m, att,
    s1, v1, s2, v2, s3, v3, s4, v4, s5, v5, s6, v6,
):
    nq = queries.shape[1]
    width = queries.shape[2]
    pix = pixels.shape[1]
    me = lax.axis_index("space")
    core = lax.rem(me, 2)
    z = lax.rem(me // 2, NZ)
    x = me // (2 * NZ)
    factor = math.log2(math.e) / math.sqrt(HEAD)

    def at(xx, zz, cc):
        return {"space": (xx * NZ + zz) * 2 + cc}

    def x_peer(d):
        return at(lax.rem(x + d, NX), z, core)

    def z_peer(d):
        return at(x, lax.rem(z + d, NZ), core)

    partner = at(x, z, 1 - core)

    barrier = pltpu.get_barrier_semaphore()
    pl.semaphore_signal(barrier, inc=1, device_id=partner, device_id_type=MESH)
    for d in range(1, NX):
        pl.semaphore_signal(barrier, inc=1, device_id=x_peer(d), device_id_type=MESH)
    for d in range(1, NZ):
        pl.semaphore_signal(barrier, inc=1, device_id=z_peer(d), device_id_type=MESH)

    def image_loads(i):
        pairs = ((pixels_in, pixels), (queries_in, queries), (masks_in, masks))
        return [pltpu.make_async_copy(a.at[i], b.at[i], image_sem.at[i, k]) for k, (a, b) in enumerate(pairs)]

    early = [
        pltpu.make_async_copy(a, b, early_sem.at[k])
        for k, (a, b) in enumerate(
            ((wq_in, wq), (wv_in, wv), (wk_in, wk), (pixel_pos_in, pixel_pos), (query_pos_in, query_pos))
        )
    ]
    late = [
        pltpu.make_async_copy(a, b, late_sem.at[k])
        for k, (a, b) in enumerate(
            (
                (wo_in, wo), (gain_cross_in, gain_cross), (w_qkv_in, w_qkv), (wo_self_in, wo_self),
                (gain_self_in, gain_self), (w_in_in, w_in), (w_out_in, w_out), (gain_ffn_in, gain_ffn),
            )
        )
    ]
    for copy in early:
        copy.start()
    for group in (1 - core, core):
        for j in range(NX):
            for copy in image_loads(group * NX + lax.rem(x + j + 1, NX)):
                copy.start()
    for copy in late:
        copy.start()

    def send(src, dst, send_sem, recv_sem, where):
        return pltpu.make_async_remote_copy(
            src_ref=src, dst_ref=dst, send_sem=send_sem, recv_sem=recv_sem, device_id=where, device_id_type=MESH
        )

    rows = lax.broadcasted_iota(jnp.int32, (pix, pix), 0)
    cols = lax.broadcasted_iota(jnp.int32, (pix, pix), 1)
    eye[...] = jnp.where(rows == cols, 1.0, 0.0).astype(BF16)
    query_t[...] = jnp.zeros_like(query_t)
    bias[...] = jnp.zeros_like(bias)
    for h in range(HEADS):
        values_t[h, HEAD:, :] = jnp.ones((16, pix), BF16)
    for copy in early:
        copy.wait()
    wq_t[...] = dot_nt(eye[...], wq[...]).astype(BF16)
    wv_t[...] = dot_nt(eye[...], wv[...]).astype(BF16)

    def partial(i, put_o, m_ref):
        for copy in image_loads(i):
            copy.wait()
        one = pixels[i]
        key_in = (one.astype(F32) + pixel_pos[...].astype(F32)).astype(BF16)
        keys[...] = dot(key_in, wk[...]).astype(BF16)
        v_t = dot_nt(wv_t[...], one).astype(BF16)
        for h in range(HEADS):
            values_t[h, :HEAD, :] = v_t[h * HEAD : (h + 1) * HEAD, :]
        query_in = (queries[i].astype(F32) + query_pos[...].astype(F32)).astype(BF16)
        query_t[:, :nq] = dot_nt(wq_t[...], query_in).astype(BF16)
        mask_t = dot_nt(eye[...], masks[i].astype(F32).astype(BF16))
        count = jnp.sum(mask_t, axis=0, keepdims=True)
        bias[:, :nq] = jnp.where((mask_t > 0.5) | (count == 0.0), 0.0, FAR)
        sign = jnp.where(count == 0.0, -1.0, 1.0)
        for h in range(HEADS):
            tile = (h // 4) * 128
            lane = (h % 4) * HEAD
            parts = []
            if lane:
                parts.append(jnp.zeros((lane, LANES), BF16))
            parts.append(query_t[h * HEAD : (h + 1) * HEAD, :])
            if lane + HEAD < 128:
                parts.append(jnp.zeros((128 - lane - HEAD, LANES), BF16))
            one_head = jnp.concatenate(parts, axis=0)
            score = dot(keys[:, tile : tile + 128], one_head) * factor + bias[...]
            scores[h] = score
            m_ref[h : h + 1, :] = jnp.max(score, axis=0, keepdims=True)
        for h in range(HEADS):
            weights[h] = jnp.exp2(scores[h] - m_ref[h : h + 1, :]).astype(BF16)
        for h in range(HEADS):
            both = dot(values_t[h], weights[h])
            put_o(h, both[:HEAD])
            m_ref[HEADS + h : HEADS + h + 1, :] = both[HEAD : HEAD + 1]
        m_ref[HEADS:, :nq] = m_ref[HEADS:, :nq] * sign

    def first(j, carry):
        i = (1 - core) * NX + lax.rem(x + j + 1, NX)

        def put(h, value):
            p1o[j, h * HEAD : (h + 1) * HEAD, :] = value.astype(BF16)

        partial(i, put, p1m.at[j])

        @pl.when(j == 0)
        def _():
            pl.semaphore_wait(barrier, NX + NZ - 1)

        send(p1o.at[j], r1o.at[j], s1.at[j, 0], v1.at[j, 0], partner).start()
        send(p1m.at[j], r1m.at[j], s1.at[j, 1], v1.at[j, 1], partner).start()
        return carry

    lax.fori_loop(0, NX, first, 0)

    def second(j, carry):
        i = core * NX + lax.rem(x + j + 1, NX)

        def put(h, value):
            own_o[h * HEAD : (h + 1) * HEAD, :] = value

        partial(i, put, own_m)
        a = send(p1o.at[j], r1o.at[j], s1.at[j, 0], v1.at[j, 0], partner)
        b = send(p1m.at[j], r1m.at[j], s1.at[j, 1], v1.at[j, 1], partner)
        a.wait()
        b.wait()
        top, total, scales = merge([own_m[:HEADS], r1m[j, :HEADS]], [own_m[HEADS:], r1m[j, HEADS:]])
        p2m[j, :HEADS] = top
        p2m[j, HEADS:] = total
        for h in range(HEADS):
            part = slice(h * HEAD, (h + 1) * HEAD)
            folded = own_o[part] * scales[0][h : h + 1] + r1o[j, part].astype(F32) * scales[1][h : h + 1]
            p2o[j, part] = folded.astype(BF16)

        @pl.when(j < NX - 1)
        def _():
            to = x_peer(j + 1)
            send(p2o.at[j], r2o.at[j], s2.at[j, 0], v2.at[j, 0], to).start()
            send(p2m.at[j], r2m.at[j], s2.at[j, 1], v2.at[j, 1], to).start()

        return carry

    lax.fori_loop(0, NX, second, 0)

    mine = NX - 1
    for j in range(NX - 1):
        to = x_peer(j + 1)
        send(p2o.at[j], r2o.at[j], s2.at[j, 0], v2.at[j, 0], to).wait()
        send(p2m.at[j], r2m.at[j], s2.at[j, 1], v2.at[j, 1], to).wait()
    tops = [p2m[mine, :HEADS]] + [r2m[j, :HEADS] for j in range(NX - 1)]
    totals = [p2m[mine, HEADS:]] + [r2m[j, HEADS:] for j in range(NX - 1)]
    top, total, scales = merge(tops, totals)
    for h in range(HEADS):
        part = slice(h * HEAD, (h + 1) * HEAD)
        folded = p2o[mine, part].astype(F32) * scales[0][h : h + 1]
        for j in range(NX - 1):
            folded = folded + r2o[j, part].astype(F32) * scales[j + 1][h : h + 1]
        p3o[h] = folded.astype(BF16)
        p3m[h, 0:1] = top[h : h + 1]
        p3m[h, 1:2] = total[h : h + 1]

    def z_send(d):
        h = lax.rem(z + d, NZ)
        return (
            send(p3o.at[h], r3o.at[d - 1], s3.at[d - 1, 0], v3.at[d - 1, 0], z_peer(d)),
            send(p3m.at[h], r3m.at[d - 1], s3.at[d - 1, 1], v3.at[d - 1, 1], z_peer(d)),
        )

    order = (4, 3, 5, 2, 6, 1, 7)
    for d in order:
        for copy in z_send(d):
            copy.start()
    for d in order[::-1]:
        for copy in z_send(d):
            copy.wait()
    tops = [p3m[z, 0:1]] + [r3m[d, 0:1] for d in range(NZ - 1)]
    totals = [p3m[z, 1:2]] + [r3m[d, 1:2] for d in range(NZ - 1)]
    top, total, scales = merge(tops, totals)
    folded = p3o[z].astype(F32) * scales[0]
    for d in range(NZ - 1):
        folded = folded + r3o[d].astype(F32) * scales[d + 1]
    att[z] = (folded / jnp.abs(total)).astype(BF16)

    def z_gather(d):
        return send(att.at[z], att.at[z], s4.at[d - 1], v4.at[d - 1], z_peer(d))

    for d in order:
        z_gather(d).start()
    for d in order[::-1]:
        z_gather(d).wait()

    i_own = core * NX + x
    for copy in late:
        copy.wait()
    attended_t = att[...].reshape(width, LANES)
    cross = dot(attended_t, wo[...], ((0,), (0,)))[:nq]
    pos = query_pos[...].astype(F32)
    after_cross = layer_norm(queries[i_own].astype(F32) + cross, gain_cross[...]).astype(BF16)
    self_in = (after_cross.astype(F32) + pos).astype(BF16)
    both = dot(self_in, w_qkv[:, : 2 * width]).astype(BF16)
    self_v = dot(after_cross, w_qkv[:, 2 * width :]).astype(BF16)
    head_of = lax.broadcasted_iota(jnp.int32, (nq, 128), 1) // HEAD
    outs = []
    for tile in range(width // 128):
        part = slice(tile * 128, (tile + 1) * 128)
        q_tile = both[:, part].astype(F32)
        k_tile = both[:, width + tile * 128 : width + (tile + 1) * 128]
        v_tile = self_v[:, part]
        gathered = jnp.zeros((nq, 128), F32)
        for h in range(128 // HEAD):
            q_head = jnp.where(head_of == h, q_tile, 0.0).astype(BF16)
            logits = dot_nt(q_head, k_tile) * (1.0 / math.sqrt(HEAD))
            top = jnp.max(logits, axis=-1, keepdims=True)
            expo = jnp.exp(logits - top)
            weight = (expo / jnp.sum(expo, axis=-1, keepdims=True)).astype(BF16)
            gathered = jnp.where(head_of == h, dot(weight, v_tile), gathered)
        outs.append(gathered.astype(BF16))
    self_proj = dot(jnp.concatenate(outs, axis=1), wo_self[...])
    after_self = layer_norm(after_cross.astype(F32) + self_proj, gain_self[...]).astype(BF16)
    halves = (slice(0, 96), slice(96, nq))

    def x_out(part, d, k):
        rows = halves[part]
        return send(out.at[i_own, rows], out.at[i_own, rows], s5.at[k], v5.at[k], x_peer(d))

    def x_pass(part, d, k):
        i = core * NX + lax.rem(x - d + NX, NX)
        rows = halves[part]
        return send(out.at[i, rows], out.at[i, rows], s5.at[k], v5.at[k], x_peer(d))

    def core_out(part, back):
        i = core * NX + lax.rem(x - back + NX, NX)
        rows = halves[part]
        k = 2 * back + part
        return send(out.at[i, rows], out.at[i, rows], s6.at[k], v6.at[k], partner)

    for part in range(2):
        rows = halves[part]
        hidden = jnp.maximum(dot(after_self[rows], w_in[...]), 0.0).astype(BF16)
        ffn = dot(hidden, w_out[...])
        out[i_own, rows] = layer_norm(after_self[rows].astype(F32) + ffn, gain_ffn[...]).astype(BF16)
        x_out(part, 1, part).start()
        x_out(part, NX - 1, 2 + part).start()
        core_out(part, 0).start()
    x_out(0, 1, 0).wait_recv()
    x_pass(0, 1, 4).start()
    core_out(0, 1).start()
    x_out(0, NX - 1, 2).wait_recv()
    core_out(0, NX - 1).start()
    x_out(1, NX - 1, 3).wait_recv()
    x_pass(1, NX - 1, 5).start()
    core_out(1, NX - 1).start()
    x_out(1, 1, 1).wait_recv()
    core_out(1, 1).start()
    x_pass(0, 1, 4).wait_recv()
    core_out(0, 2).start()
    x_pass(1, NX - 1, 5).wait_recv()
    core_out(1, 2).start()
    for part in range(2):
        x_out(part, 1, part).wait_send()
        x_out(part, NX - 1, 2 + part).wait_send()
    x_pass(0, 1, 4).wait_send()
    x_pass(1, NX - 1, 5).wait_send()
    for part in range(2):
        for back in range(NX):
            core_out(part, back).wait()


def local(
    queries, query_pos, pixels, pixel_pos, masks, wq_cross, wk_cross, wv_cross, wo_cross, gain_cross, w_qkv, wo_self,
    gain_self, w_in, w_out, gain_ffn,
):
    images, nq, width = queries.shape
    pix = pixels.shape[1]
    dma = pltpu.SemaphoreType.DMA
    vmem = pltpu.VMEM
    operands = (
        queries, query_pos, pixels, pixel_pos, masks, wq_cross, wk_cross, wv_cross, wo_cross, gain_cross[None], w_qkv,
        wo_self, gain_self[None], w_in, w_out, gain_ffn[None],
    )
    scratch = [vmem(a.shape, a.dtype) for a in operands] + [
        dma((images, 3)),
        dma((5,)),
        dma((8,)),
        vmem((width, width), BF16),
        vmem((width, width), BF16),
        vmem((pix, pix), BF16),
        vmem((pix, width), BF16),
        vmem((HEADS, HEAD + 16, pix), BF16),
        vmem((width, LANES), BF16),
        vmem((pix, LANES), F32),
        vmem((HEADS, pix, LANES), F32),
        vmem((HEADS, pix, LANES), BF16),
        vmem((width, LANES), F32),
        vmem((2 * HEADS, LANES), F32),
        vmem((NX, width, LANES), BF16),
        vmem((NX, 2 * HEADS, LANES), F32),
        vmem((NX, width, LANES), BF16),
        vmem((NX, 2 * HEADS, LANES), F32),
        vmem((NX, width, LANES), BF16),
        vmem((NX, 2 * HEADS, LANES), F32),
        vmem((NX - 1, width, LANES), BF16),
        vmem((NX - 1, 2 * HEADS, LANES), F32),
        vmem((NZ, HEAD, LANES), BF16),
        vmem((NZ, 8, LANES), F32),
        vmem((NZ - 1, HEAD, LANES), BF16),
        vmem((NZ - 1, 8, LANES), F32),
        vmem((NZ, HEAD, LANES), BF16),
        dma((NX, 2)),
        dma((NX, 2)),
        dma((NX - 1, 2)),
        dma((NX - 1, 2)),
        dma((NZ - 1, 2)),
        dma((NZ - 1, 2)),
        dma((NZ - 1,)),
        dma((NZ - 1,)),
        dma((6,)),
        dma((6,)),
        dma((2 * NX,)),
        dma((2 * NX,)),
    ]
    return pl.pallas_call(
        kernel,
        out_shape=jax.ShapeDtypeStruct((images, nq, width), BF16),
        in_specs=[pl.BlockSpec(memory_space=pltpu.HBM)] * 16,
        out_specs=pl.BlockSpec(memory_space=pltpu.VMEM),
        scratch_shapes=scratch,
        compiler_params=pltpu.CompilerParams(
            collective_id=0, has_side_effects=True, vmem_limit_bytes=67043328
        ),
        name="decoder_layer",
    )(*operands)


def solution(mesh):
    placed = (
        P("dp", None, None),
        P(),
        P("dp", "space", None),
        P("space", None),
        P("dp", None, "space"),
    ) + (P(),) * 11
    return jax.shard_map(local, mesh=mesh, in_specs=placed, out_specs=P("dp", None, None), check_vma=False)
```

```python
import math

import jax
import jax.numpy as jnp
from jax import lax
from jax.experimental import pallas as pl
from jax.experimental.pallas import tpu as pltpu
from jax.sharding import PartitionSpec as P

HEADS = 8
HEAD = 32
NX = 4
NZ = 8
LANES = 256
FAR = -1e30
MESH = pl.DeviceIdType.MESH
F32 = jnp.float32
BF16 = jnp.bfloat16


def dot(a, b, contract=((1,), (0,))):
    return lax.dot_general(a, b, (contract, ((), ())), preferred_element_type=F32)


def dot_nt(a, b):
    return dot(a, b, ((1,), (1,)))


def layer_norm(x, gain):
    mean = jnp.mean(x, axis=-1, keepdims=True)
    d = x - mean
    var = jnp.mean(d * d, axis=-1, keepdims=True)
    return d / jnp.sqrt(var + 1e-05) * gain


def merge(tops, totals):
    most = totals[0]
    for t in totals[1:]:
        most = jnp.maximum(most, t)
    some = most > 0
    seen = [jnp.where(some & (t < 0), -3e38, m) for m, t in zip(tops, totals)]
    top = seen[0]
    for m in seen[1:]:
        top = jnp.maximum(top, m)
    scales = [jnp.exp2(m - top) for m in seen]
    total = scales[0] * jnp.abs(totals[0])
    for s, t in zip(scales[1:], totals[1:]):
        total = total + s * jnp.abs(t)
    return top, jnp.where(some, total, -total), scales


def kernel(
    queries_in, query_pos_in, pixels_in, pixel_pos_in, masks_in, wq_in, wk_in, wv_in, wo_in, gain_cross_in, w_qkv_in,
    wo_self_in, gain_self_in, w_in_in, w_out_in, gain_ffn_in,
    out,
    queries, query_pos, pixels, pixel_pos, masks, wq, wk, wv, wo, gain_cross, w_qkv, wo_self, gain_self, w_in, w_out,
    gain_ffn, image_sem, early_sem, late_sem,
    wq_t, wv_t, eye, keys_a, values_a, query_a, bias_a, keys_b, values_b, query_b, bias_b, scores, weights, own_o, own_m,
    p1o, p1m, r1o, r1m, p2o, p2m, r2o, r2m, p3o, p3m, r3o, r3m, att,
    mine_out, around,
    s1, v1, s2, v2, s3, v3, s4, v4, s5, v5, s6, v6, store_sem,
):
    nq = queries.shape[1]
    width = queries.shape[2]
    pix = pixels.shape[1]
    me = lax.axis_index("space")
    core = lax.rem(me, 2)
    z = lax.rem(me // 2, NZ)
    x = me // (2 * NZ)
    factor = math.log2(math.e) / math.sqrt(HEAD)

    def at(xx, zz, cc):
        return {"space": (xx * NZ + zz) * 2 + cc}

    def x_peer(d):
        return at(lax.rem(x + d, NX), z, core)

    def z_peer(d):
        return at(x, lax.rem(z + d, NZ), core)

    partner = at(x, z, 1 - core)

    def image_loads(i):
        pairs = ((pixels_in, pixels), (queries_in, queries), (masks_in, masks))
        return [pltpu.make_async_copy(a.at[i], b.at[i], image_sem.at[i, k]) for k, (a, b) in enumerate(pairs)]

    early = [
        pltpu.make_async_copy(a, b, early_sem.at[k])
        for k, (a, b) in enumerate(
            ((wq_in, wq), (wv_in, wv), (wk_in, wk), (pixel_pos_in, pixel_pos), (query_pos_in, query_pos))
        )
    ]
    late = [
        pltpu.make_async_copy(a, b, late_sem.at[k])
        for k, (a, b) in enumerate(
            (
                (wo_in, wo), (gain_cross_in, gain_cross), (w_qkv_in, w_qkv), (wo_self_in, wo_self),
                (gain_self_in, gain_self), (w_in_in, w_in), (w_out_in, w_out), (gain_ffn_in, gain_ffn),
            )
        )
    ]
    for copy in early:
        copy.start()
    for j in range(NX):
        for group in (1 - core, core):
            for copy in image_loads(group * NX + lax.rem(x + j + 1, NX)):
                copy.start()

    barrier = pltpu.get_barrier_semaphore()
    pl.semaphore_signal(barrier, inc=1, device_id=partner, device_id_type=MESH)
    for d in range(1, NX):
        pl.semaphore_signal(barrier, inc=1, device_id=x_peer(d), device_id_type=MESH)
    for d in range(1, NZ):
        pl.semaphore_signal(barrier, inc=1, device_id=z_peer(d), device_id_type=MESH)

    def send(src, dst, send_sem, recv_sem, where):
        return pltpu.make_async_remote_copy(
            src_ref=src, dst_ref=dst, send_sem=send_sem, recv_sem=recv_sem, device_id=where, device_id_type=MESH
        )

    rows = lax.broadcasted_iota(jnp.int32, (pix, pix), 0)
    cols = lax.broadcasted_iota(jnp.int32, (pix, pix), 1)
    eye[...] = jnp.where(rows == cols, 1.0, 0.0).astype(BF16)
    theirs = (keys_a, values_a, query_a, bias_a)
    ours = (keys_b, values_b, query_b, bias_b)
    for _, values_t, query_t, bias in (theirs, ours):
        query_t[...] = jnp.zeros_like(query_t)
        bias[:pix] = jnp.zeros((pix, LANES), F32)
        bias[pix:] = jnp.ones((8, LANES), F32)
        for h in range(HEADS):
            values_t[h, HEAD:, :] = jnp.ones((16, pix), BF16)
    for copy in early:
        copy.wait()
    wq_t[...] = dot_nt(eye[...], wq[...]).astype(BF16)
    wv_t[...] = dot_nt(eye[...], wv[...]).astype(BF16)

    def prepare(i, bufs):
        keys, values_t, query_t, bias = bufs

        def key_piece():
            key_in = (pixels[i].astype(F32) + pixel_pos[...].astype(F32)).astype(BF16)
            keys[...] = dot(key_in, wk[...]).astype(BF16)

        def value_piece():
            v_t = dot_nt(wv_t[...], pixels[i]).astype(BF16)
            for h in range(HEADS):
                values_t[h, :HEAD, :] = v_t[h * HEAD : (h + 1) * HEAD, :]

        def query_piece():
            query_in = (queries[i].astype(F32) + query_pos[...].astype(F32)).astype(BF16)
            query_t[:, :nq] = dot_nt(wq_t[...], query_in).astype(BF16)

        def mask_piece():
            mask_t = dot_nt(eye[...], masks[i].astype(F32).astype(BF16))
            count = jnp.sum(mask_t, axis=0, keepdims=True)
            bias[:pix, :nq] = jnp.where((mask_t > 0.5) | (count == 0.0), 0.0, FAR)
            bias[pix : pix + 1, :nq] = jnp.where(count == 0.0, -1.0, 1.0)

        return [key_piece, value_piece, query_piece, mask_piece]

    def attend(bufs, put_o, m_ref, pieces):
        keys, values_t, query_t, bias = bufs
        for h in range(HEADS):
            tile = (h // 4) * 128
            lane = (h % 4) * HEAD
            parts = []
            if lane:
                parts.append(jnp.zeros((lane, LANES), BF16))
            parts.append(query_t[h * HEAD : (h + 1) * HEAD, :])
            if lane + HEAD < 128:
                parts.append(jnp.zeros((128 - lane - HEAD, LANES), BF16))
            one_head = jnp.concatenate(parts, axis=0)
            score = dot(keys[:, tile : tile + 128], one_head) * factor + bias[:pix]
            scores[h] = score
            m_ref[h : h + 1, :] = jnp.max(score, axis=0, keepdims=True)
            if pieces and h % 2 == 1:
                pieces[h // 2]()
        for h in range(HEADS):
            weights[h] = jnp.exp2(scores[h] - m_ref[h : h + 1, :]).astype(BF16)
        for h in range(HEADS):
            both = dot(values_t[h], weights[h])
            put_o(h, both[:HEAD])
            m_ref[HEADS + h : HEADS + h + 1, :] = both[HEAD : HEAD + 1] * bias[pix : pix + 1]

    def turn(j, cc):
        first = j // (NX - 1)
        second = lax.rem(j, 2) * (1 - first)
        return 2 * (1 - (j + 2) // (NX - 1)) + (1 + 2 * cc) * second + (3 - 2 * cc) * (j // 2) * (1 - first)

    def image(j, cc):
        return cc * NX + lax.rem(x + turn(j, cc), NX)

    def arrived(i):
        for copy in image_loads(i):
            copy.wait()

    arrived(image(0, 1 - core))
    for piece in prepare(image(0, 1 - core), theirs):
        piece()

    def step(j, carry):
        far = turn(j, core)

        def put(h, value):
            p1o[j, h * HEAD : (h + 1) * HEAD, :] = value.astype(BF16)

        arrived(image(j, core))
        attend(theirs, put, p1m.at[j], prepare(image(j, core), ours))

        @pl.when(j == 0)
        def _():
            pl.semaphore_wait(barrier, NX + NZ - 1)
            for copy in late:
                copy.start()

        a = send(p1o.at[j], r1o.at[j], s1.at[j, 0], v1.at[j, 0], partner)
        b = send(p1m.at[j], r1m.at[j], s1.at[j, 1], v1.at[j, 1], partner)
        a.start()
        b.start()

        def put_own(h, value):
            own_o[h * HEAD : (h + 1) * HEAD, :] = value

        following = image(jnp.minimum(j + 1, NX - 1), 1 - core)

        @pl.when(j < NX - 1)
        def _():
            arrived(following)

        attend(ours, put_own, own_m, prepare(following, theirs))
        a.wait()
        b.wait()
        top, total, scales = merge([own_m[:HEADS], r1m[j, :HEADS]], [own_m[HEADS:], r1m[j, HEADS:]])
        p2m[far, :HEADS] = top
        p2m[far, HEADS:] = total
        for h in range(HEADS):
            part = slice(h * HEAD, (h + 1) * HEAD)
            folded = own_o[part] * scales[0][h : h + 1] + r1o[j, part].astype(F32) * scales[1][h : h + 1]
            p2o[far, part] = folded.astype(BF16)

        @pl.when(j < NX - 1)
        def _():
            for copy in x_send(far):
                copy.start()

        return carry

    def x_send(far):
        k = far - 1
        return (
            send(p2o.at[far], r2o.at[k], s2.at[k, 0], v2.at[k, 0], x_peer(far)),
            send(p2m.at[far], r2m.at[k], s2.at[k, 1], v2.at[k, 1], x_peer(far)),
        )

    lax.fori_loop(0, NX, step, 0)

    mine = 0
    for far in range(1, NX):
        for copy in x_send(far):
            copy.wait()
    tops = [p2m[mine, :HEADS]] + [r2m[j, :HEADS] for j in range(NX - 1)]
    totals = [p2m[mine, HEADS:]] + [r2m[j, HEADS:] for j in range(NX - 1)]
    top, total, scales = merge(tops, totals)
    for h in range(HEADS):
        part = slice(h * HEAD, (h + 1) * HEAD)
        folded = p2o[mine, part].astype(F32) * scales[0][h : h + 1]
        for j in range(NX - 1):
            folded = folded + r2o[j, part].astype(F32) * scales[j + 1][h : h + 1]
        p3o[h] = folded.astype(BF16)
        for k, value in enumerate((top, total)):
            p3m[h, 2 * k : 2 * k + 1] = value[h : h + 1, :128]
            p3m[h, 2 * k + 1 : 2 * k + 2] = value[h : h + 1, 128:]

    def z_send(d):
        h = lax.rem(z + d, NZ)
        return (
            send(p3o.at[h], r3o.at[d - 1], s3.at[d - 1, 0], v3.at[d - 1, 0], z_peer(d)),
            send(p3m.at[h], r3m.at[d - 1], s3.at[d - 1, 1], v3.at[d - 1, 1], z_peer(d)),
        )

    order = (4, 3, 5, 2, 6, 1, 7)
    for d in order:
        for copy in z_send(d):
            copy.start()
    for d in order[::-1]:
        for copy in z_send(d):
            copy.wait()

    def wide(ref, k, which):
        return jnp.concatenate([ref[k, 2 * which : 2 * which + 1], ref[k, 2 * which + 1 : 2 * which + 2]], axis=1)

    tops = [wide(p3m, z, 0)] + [wide(r3m, d, 0) for d in range(NZ - 1)]
    totals = [wide(p3m, z, 1)] + [wide(r3m, d, 1) for d in range(NZ - 1)]
    top, total, scales = merge(tops, totals)
    folded = p3o[z].astype(F32) * scales[0]
    for d in range(NZ - 1):
        folded = folded + r3o[d].astype(F32) * scales[d + 1]
    att[z] = (folded / jnp.abs(total)).astype(BF16)

    def z_gather(d):
        return send(att.at[z], att.at[z], s4.at[d - 1], v4.at[d - 1], z_peer(d))

    for d in order:
        z_gather(d).start()
    for d in order[::-1]:
        z_gather(d).wait()

    i_own = core * NX + x
    for copy in late:
        copy.wait()
    attended_t = att[...].reshape(width, LANES)
    cross = dot(attended_t, wo[...], ((0,), (0,)))[:nq]
    pos = query_pos[...].astype(F32)
    after_cross = layer_norm(queries[i_own].astype(F32) + cross, gain_cross[...]).astype(BF16)
    self_in = (after_cross.astype(F32) + pos).astype(BF16)
    both = dot(self_in, w_qkv[:, : 2 * width]).astype(BF16)
    self_v = dot(after_cross, w_qkv[:, 2 * width :]).astype(BF16)
    head_of = lax.broadcasted_iota(jnp.int32, (nq, 128), 1) // HEAD
    outs = []
    for tile in range(width // 128):
        part = slice(tile * 128, (tile + 1) * 128)
        q_tile = both[:, part].astype(F32)
        k_tile = both[:, width + tile * 128 : width + (tile + 1) * 128]
        v_tile = self_v[:, part]
        gathered = jnp.zeros((nq, 128), F32)
        for h in range(128 // HEAD):
            q_head = jnp.where(head_of == h, q_tile, 0.0).astype(BF16)
            logits = dot_nt(q_head, k_tile) * (1.0 / math.sqrt(HEAD))
            top = jnp.max(logits, axis=-1, keepdims=True)
            expo = jnp.exp(logits - top)
            weight = (expo / jnp.sum(expo, axis=-1, keepdims=True)).astype(BF16)
            gathered = jnp.where(head_of == h, dot(weight, v_tile), gathered)
        outs.append(gathered.astype(BF16))
    self_proj = dot(jnp.concatenate(outs, axis=1), wo_self[...])
    after_self = layer_norm(after_cross.astype(F32) + self_proj, gain_self[...]).astype(BF16)
    halves = (slice(0, 96), slice(96, nq))

    def x_out(part, d):
        rows = halves[part]
        k = 2 * (d // 2) + part
        return send(mine_out.at[rows], around.at[d - 1, rows], s5.at[k], v5.at[k], x_peer(d))

    def x_pass(part):
        rows = halves[part]
        back, d = ((1, 1), (NX - 1, NX - 1))[part]
        return send(around.at[back - 1, rows], around.at[1, rows], s5.at[4 + part], v5.at[4 + part], x_peer(d))

    def finish(part, back):
        rows = halves[part]
        k = 2 * back + part
        i = core * NX + lax.rem(x - back + NX, NX)
        source = mine_out.at[rows] if back == 0 else around.at[back - 1, rows]
        return (
            pltpu.make_async_copy(source, out.at[i, rows], store_sem.at[k]),
            send(source, out.at[i, rows], s6.at[k], v6.at[k], partner),
        )

    def pass_on(part, back):
        for copy in finish(part, back)[::-1]:
            copy.start()

    for part in range(2):
        rows = halves[part]
        hidden = jnp.maximum(dot(after_self[rows], w_in[...]), 0.0).astype(BF16)
        ffn = dot(hidden, w_out[...])
        mine_out[rows] = layer_norm(after_self[rows].astype(F32) + ffn, gain_ffn[...]).astype(BF16)
        x_out(part, 1).start()
        x_out(part, NX - 1).start()
        pass_on(part, 0)
    x_out(0, 1).wait_recv()
    x_pass(0).start()
    pass_on(0, 1)
    x_out(0, NX - 1).wait_recv()
    pass_on(0, NX - 1)
    x_out(1, NX - 1).wait_recv()
    x_pass(1).start()
    pass_on(1, NX - 1)
    x_out(1, 1).wait_recv()
    pass_on(1, 1)
    x_pass(0).wait_recv()
    pass_on(0, 2)
    x_pass(1).wait_recv()
    pass_on(1, 2)
    for part in range(2):
        x_out(part, 1).wait_send()
        x_out(part, NX - 1).wait_send()
        x_pass(part).wait_send()
        for back in range(NX):
            for copy in finish(part, back):
                copy.wait()


def local(
    queries, query_pos, pixels, pixel_pos, masks, wq_cross, wk_cross, wv_cross, wo_cross, gain_cross, w_qkv, wo_self,
    gain_self, w_in, w_out, gain_ffn,
):
    images, nq, width = queries.shape
    pix = pixels.shape[1]
    dma = pltpu.SemaphoreType.DMA
    vmem = pltpu.VMEM
    operands = (
        queries, query_pos, pixels, pixel_pos, masks, wq_cross, wk_cross, wv_cross, wo_cross, gain_cross[None], w_qkv,
        wo_self, gain_self[None], w_in, w_out, gain_ffn[None],
    )
    scratch = [vmem(a.shape, a.dtype) for a in operands] + [
        dma((images, 3)),
        dma((5,)),
        dma((8,)),
        vmem((width, width), BF16),
        vmem((width, width), BF16),
        vmem((pix, pix), BF16),
        vmem((pix, width), BF16),
        vmem((HEADS, HEAD + 16, pix), BF16),
        vmem((width, LANES), BF16),
        vmem((pix + 8, LANES), F32),
        vmem((pix, width), BF16),
        vmem((HEADS, HEAD + 16, pix), BF16),
        vmem((width, LANES), BF16),
        vmem((pix + 8, LANES), F32),
        vmem((HEADS, pix, LANES), F32),
        vmem((HEADS, pix, LANES), BF16),
        vmem((width, LANES), F32),
        vmem((2 * HEADS, LANES), F32),
        vmem((NX, width, LANES), BF16),
        vmem((NX, 2 * HEADS, LANES), F32),
        vmem((NX, width, LANES), BF16),
        vmem((NX, 2 * HEADS, LANES), F32),
        vmem((NX, width, LANES), BF16),
        vmem((NX, 2 * HEADS, LANES), F32),
        vmem((NX - 1, width, LANES), BF16),
        vmem((NX - 1, 2 * HEADS, LANES), F32),
        vmem((NZ, HEAD, LANES), BF16),
        vmem((NZ, 8, 128), F32),
        vmem((NZ - 1, HEAD, LANES), BF16),
        vmem((NZ - 1, 8, 128), F32),
        vmem((NZ, HEAD, LANES), BF16),
        vmem((nq, width), BF16),
        vmem((NX - 1, nq, width), BF16),
        dma((NX, 2)),
        dma((NX, 2)),
        dma((NX - 1, 2)),
        dma((NX - 1, 2)),
        dma((NZ - 1, 2)),
        dma((NZ - 1, 2)),
        dma((NZ - 1,)),
        dma((NZ - 1,)),
        dma((6,)),
        dma((6,)),
        dma((2 * NX,)),
        dma((2 * NX,)),
        dma((2 * NX,)),
    ]
    return pl.pallas_call(
        kernel,
        out_shape=jax.ShapeDtypeStruct((images, nq, width), BF16),
        in_specs=[pl.BlockSpec(memory_space=pltpu.HBM)] * 16,
        out_specs=pl.BlockSpec(memory_space=pltpu.HBM),
        scratch_shapes=scratch,
        compiler_params=pltpu.CompilerParams(
            collective_id=0, has_side_effects=True, vmem_limit_bytes=67043328
        ),
        name="decoder_layer",
    )(*operands)


def solution(mesh):
    placed = (
        P("dp", None, None),
        P(),
        P("dp", "space", None),
        P("space", None),
        P("dp", None, "space"),
    ) + (P(),) * 11
    return jax.shard_map(local, mesh=mesh, in_specs=placed, out_specs=P("dp", None, None), check_vma=False)
```

```python
import math

import jax
import jax.numpy as jnp
from jax import lax
from jax.experimental import pallas as pl
from jax.experimental.pallas import tpu as pltpu
from jax.sharding import PartitionSpec as P

HEADS = 8
HEAD = 32
NX = 4
NZ = 8
LANES = 256
FAR = -1e30
MESH = pl.DeviceIdType.MESH
F32 = jnp.float32
BF16 = jnp.bfloat16


def dot(a, b, contract=((1,), (0,))):
    return lax.dot_general(a, b, (contract, ((), ())), preferred_element_type=F32)


def dot_nt(a, b):
    return dot(a, b, ((1,), (1,)))


def layer_norm(x, gain):
    mean = jnp.mean(x, axis=-1, keepdims=True)
    d = x - mean
    var = jnp.mean(d * d, axis=-1, keepdims=True)
    return d / jnp.sqrt(var + 1e-05) * gain


def merge(tops, totals):
    most = totals[0]
    for t in totals[1:]:
        most = jnp.maximum(most, t)
    some = most > 0
    seen = [jnp.where(some & (t < 0), -3e38, m) for m, t in zip(tops, totals)]
    top = seen[0]
    for m in seen[1:]:
        top = jnp.maximum(top, m)
    scales = [jnp.exp2(m - top) for m in seen]
    total = scales[0] * jnp.abs(totals[0])
    for s, t in zip(scales[1:], totals[1:]):
        total = total + s * jnp.abs(t)
    return top, jnp.where(some, total, -total), scales


def kernel(
    queries_in, query_pos_in, pixels_in, pixel_pos_in, masks_in, wq_in, wk_in, wv_in, wo_in, gain_cross_in, w_qkv_in,
    wo_self_in, gain_self_in, w_in_in, w_out_in, gain_ffn_in,
    out,
    queries, query_pos, pixels, pixel_pos, masks, wq, wk, wv, wo, gain_cross, w_qkv, wo_self, gain_self, w_in, w_out,
    gain_ffn, image_sem, early_sem, late_sem,
    wq_t, wv_t, eye, keys_a, values_a, query_a, bias_a, keys_b, values_b, query_b, bias_b, scores, weights, own_o, own_m,
    p1o, p1m, r1o, r1m, p2o, p2m, r2o, r2m, p3o, p3m, r3o, r3m, att,
    mine_out, around,
    s1, v1, s2, v2, s3, v3, s4, v4, s5, v5, s6, v6, store_sem,
):
    nq = queries.shape[1]
    width = queries.shape[2]
    pix = pixels.shape[1]
    me = lax.axis_index("space")
    core = lax.rem(me, 2)
    z = lax.rem(me // 2, NZ)
    x = me // (2 * NZ)
    factor = math.log2(math.e) / math.sqrt(HEAD)

    def at(xx, zz, cc):
        return {"space": (xx * NZ + zz) * 2 + cc}

    def x_peer(d):
        return at(lax.rem(x + d, NX), z, core)

    def z_peer(d):
        return at(x, lax.rem(z + d, NZ), core)

    partner = at(x, z, 1 - core)

    def image_loads(i):
        pairs = ((pixels_in, pixels), (queries_in, queries), (masks_in, masks))
        return [pltpu.make_async_copy(a.at[i], b.at[i], image_sem.at[i, k]) for k, (a, b) in enumerate(pairs)]

    early = [
        pltpu.make_async_copy(a, b, early_sem.at[k])
        for k, (a, b) in enumerate(
            ((wq_in, wq), (wv_in, wv), (wk_in, wk), (pixel_pos_in, pixel_pos), (query_pos_in, query_pos))
        )
    ]
    late = [
        pltpu.make_async_copy(a, b, late_sem.at[k])
        for k, (a, b) in enumerate(
            (
                (wo_in, wo), (gain_cross_in, gain_cross), (w_qkv_in, w_qkv), (wo_self_in, wo_self),
                (gain_self_in, gain_self), (w_in_in, w_in), (w_out_in, w_out), (gain_ffn_in, gain_ffn),
            )
        )
    ]
    for copy in early:
        copy.start()
    def turn(j, cc):
        first = j // (NX - 1)
        second = lax.rem(j, 2) * (1 - first)
        return 2 * (1 - (j + 2) // (NX - 1)) + (1 + 2 * cc) * second + (3 - 2 * cc) * (j // 2) * (1 - first)

    def image(j, cc):
        return cc * NX + lax.rem(x + turn(j, cc), NX)

    def fetch(j, cc):
        for copy in image_loads(image(j, cc)):
            copy.start()

    fetch(0, 1 - core)
    fetch(0, core)

    barrier = pltpu.get_barrier_semaphore()
    pl.semaphore_signal(barrier, inc=1, device_id=partner, device_id_type=MESH)
    for d in range(1, NX):
        pl.semaphore_signal(barrier, inc=1, device_id=x_peer(d), device_id_type=MESH)
    for d in range(1, NZ):
        pl.semaphore_signal(barrier, inc=1, device_id=z_peer(d), device_id_type=MESH)

    def send(src, dst, send_sem, recv_sem, where):
        return pltpu.make_async_remote_copy(
            src_ref=src, dst_ref=dst, send_sem=send_sem, recv_sem=recv_sem, device_id=where, device_id_type=MESH
        )

    rows = lax.broadcasted_iota(jnp.int32, (pix, pix), 0)
    cols = lax.broadcasted_iota(jnp.int32, (pix, pix), 1)
    eye[...] = jnp.where(rows == cols, 1.0, 0.0).astype(BF16)
    theirs = (keys_a, values_a, query_a, bias_a)
    ours = (keys_b, values_b, query_b, bias_b)
    for _, values_t, query_t, bias in (theirs, ours):
        query_t[...] = jnp.zeros_like(query_t)
        bias[:pix] = jnp.zeros((pix, LANES), F32)
        bias[pix:] = jnp.ones((8, LANES), F32)
        for h in range(HEADS):
            values_t[h, HEAD:, :] = jnp.ones((16, pix), BF16)
    for copy in early:
        copy.wait()
    for j in range(1, NX):
        fetch(j, 1 - core)
        fetch(j, core)
    wq_t[...] = dot_nt(eye[...], wq[...]).astype(BF16)
    wv_t[...] = dot_nt(eye[...], wv[...]).astype(BF16)

    def prepare(i, bufs):
        keys, values_t, query_t, bias = bufs

        def key_piece():
            key_in = (pixels[i].astype(F32) + pixel_pos[...].astype(F32)).astype(BF16)
            keys[...] = dot(key_in, wk[...]).astype(BF16)

        def value_piece():
            v_t = dot_nt(wv_t[...], pixels[i]).astype(BF16)
            for h in range(HEADS):
                values_t[h, :HEAD, :] = v_t[h * HEAD : (h + 1) * HEAD, :]

        def query_piece():
            query_in = (queries[i].astype(F32) + query_pos[...].astype(F32)).astype(BF16)
            query_t[:, :nq] = dot_nt(wq_t[...], query_in).astype(BF16)

        def mask_piece():
            mask_t = dot_nt(eye[...], masks[i].astype(F32).astype(BF16))
            count = jnp.sum(mask_t, axis=0, keepdims=True)
            bias[:pix, :nq] = jnp.where((mask_t > 0.5) | (count == 0.0), 0.0, FAR)
            bias[pix : pix + 1, :nq] = jnp.where(count == 0.0, -1.0, 1.0)

        return [key_piece, value_piece, query_piece, mask_piece]

    def attend(bufs, put_o, m_ref, pieces):
        keys, values_t, query_t, bias = bufs
        for h in range(HEADS):
            tile = (h // 4) * 128
            lane = (h % 4) * HEAD
            parts = []
            if lane:
                parts.append(jnp.zeros((lane, LANES), BF16))
            parts.append(query_t[h * HEAD : (h + 1) * HEAD, :])
            if lane + HEAD < 128:
                parts.append(jnp.zeros((128 - lane - HEAD, LANES), BF16))
            one_head = jnp.concatenate(parts, axis=0)
            score = dot(keys[:, tile : tile + 128], one_head) * factor + bias[:pix]
            scores[h] = score
            m_ref[h : h + 1, :] = jnp.max(score, axis=0, keepdims=True)
            if pieces and h % 2 == 1:
                pieces[h // 2]()
        for h in range(HEADS):
            weights[h] = jnp.exp2(scores[h] - m_ref[h : h + 1, :]).astype(BF16)
        for h in range(HEADS):
            both = dot(values_t[h], weights[h])
            put_o(h, both[:HEAD])
            m_ref[HEADS + h : HEADS + h + 1, :] = both[HEAD : HEAD + 1] * bias[pix : pix + 1]

    def arrived(i):
        for copy in image_loads(i):
            copy.wait()

    arrived(image(0, 1 - core))
    for piece in prepare(image(0, 1 - core), theirs):
        piece()

    def step(j, carry):
        far = turn(j, core)

        def put(h, value):
            p1o[j, h * HEAD : (h + 1) * HEAD, :] = value.astype(BF16)

        arrived(image(j, core))
        attend(theirs, put, p1m.at[j], prepare(image(j, core), ours))

        @pl.when(j == 0)
        def _():
            pl.semaphore_wait(barrier, NX + NZ - 1)
            for copy in late:
                copy.start()

        a = send(p1o.at[j], r1o.at[j], s1.at[j, 0], v1.at[j, 0], partner)
        b = send(p1m.at[j], r1m.at[j], s1.at[j, 1], v1.at[j, 1], partner)
        a.start()
        b.start()

        def put_own(h, value):
            own_o[h * HEAD : (h + 1) * HEAD, :] = value

        following = image(jnp.minimum(j + 1, NX - 1), 1 - core)

        @pl.when(j < NX - 1)
        def _():
            arrived(following)

        attend(ours, put_own, own_m, prepare(following, theirs))
        a.wait()
        b.wait()
        top, total, scales = merge([own_m[:HEADS], r1m[j, :HEADS]], [own_m[HEADS:], r1m[j, HEADS:]])
        p2m[far, :HEADS] = top
        p2m[far, HEADS:] = total
        for h in range(HEADS):
            part = slice(h * HEAD, (h + 1) * HEAD)
            folded = own_o[part] * scales[0][h : h + 1] + r1o[j, part].astype(F32) * scales[1][h : h + 1]
            p2o[far, part] = folded.astype(BF16)

        @pl.when(j < NX - 1)
        def _():
            for copy in x_send(far):
                copy.start()

        return carry

    def x_send(far):
        k = far - 1
        return (
            send(p2o.at[far], r2o.at[k], s2.at[k, 0], v2.at[k, 0], x_peer(far)),
            send(p2m.at[far], r2m.at[k], s2.at[k, 1], v2.at[k, 1], x_peer(far)),
        )

    lax.fori_loop(0, NX, step, 0)

    mine = 0
    for far in range(1, NX):
        for copy in x_send(far):
            copy.wait()
    tops = [p2m[mine, :HEADS]] + [r2m[j, :HEADS] for j in range(NX - 1)]
    totals = [p2m[mine, HEADS:]] + [r2m[j, HEADS:] for j in range(NX - 1)]
    top, total, scales = merge(tops, totals)
    for h in range(HEADS):
        part = slice(h * HEAD, (h + 1) * HEAD)
        folded = p2o[mine, part].astype(F32) * scales[0][h : h + 1]
        for j in range(NX - 1):
            folded = folded + r2o[j, part].astype(F32) * scales[j + 1][h : h + 1]
        p3o[h] = folded.astype(BF16)
        for k, value in enumerate((top, total)):
            p3m[h, 2 * k : 2 * k + 1] = value[h : h + 1, :128]
            p3m[h, 2 * k + 1 : 2 * k + 2] = value[h : h + 1, 128:]

    def z_send(d):
        h = lax.rem(z + d, NZ)
        return (
            send(p3o.at[h], r3o.at[d - 1], s3.at[d - 1, 0], v3.at[d - 1, 0], z_peer(d)),
            send(p3m.at[h], r3m.at[d - 1], s3.at[d - 1, 1], v3.at[d - 1, 1], z_peer(d)),
        )

    order = (4, 3, 5, 2, 6, 1, 7)
    for d in order:
        for copy in z_send(d):
            copy.start()
    for d in order[::-1]:
        for copy in z_send(d):
            copy.wait()

    def wide(ref, k, which):
        return jnp.concatenate([ref[k, 2 * which : 2 * which + 1], ref[k, 2 * which + 1 : 2 * which + 2]], axis=1)

    tops = [wide(p3m, z, 0)] + [wide(r3m, d, 0) for d in range(NZ - 1)]
    totals = [wide(p3m, z, 1)] + [wide(r3m, d, 1) for d in range(NZ - 1)]
    top, total, scales = merge(tops, totals)
    folded = p3o[z].astype(F32) * scales[0]
    for d in range(NZ - 1):
        folded = folded + r3o[d].astype(F32) * scales[d + 1]
    att[z] = (folded / jnp.abs(total)).astype(BF16)

    def z_gather(d):
        return send(att.at[z], att.at[z], s4.at[d - 1], v4.at[d - 1], z_peer(d))

    for d in order:
        z_gather(d).start()
    for d in order[::-1]:
        z_gather(d).wait()

    i_own = core * NX + x
    for copy in late:
        copy.wait()
    attended_t = att[...].reshape(width, LANES)
    cross = dot(attended_t, wo[...], ((0,), (0,)))[:nq]
    pos = query_pos[...].astype(F32)
    after_cross = layer_norm(queries[i_own].astype(F32) + cross, gain_cross[...]).astype(BF16)
    self_in = (after_cross.astype(F32) + pos).astype(BF16)
    both = dot(self_in, w_qkv[:, : 2 * width]).astype(BF16)
    self_v = dot(after_cross, w_qkv[:, 2 * width :]).astype(BF16)
    head_of = lax.broadcasted_iota(jnp.int32, (nq, 128), 1) // HEAD
    outs = []
    for tile in range(width // 128):
        part = slice(tile * 128, (tile + 1) * 128)
        q_tile = both[:, part].astype(F32)
        k_tile = both[:, width + tile * 128 : width + (tile + 1) * 128]
        v_tile = self_v[:, part]
        gathered = jnp.zeros((nq, 128), F32)
        for h in range(128 // HEAD):
            q_head = jnp.where(head_of == h, q_tile, 0.0).astype(BF16)
            logits = dot_nt(q_head, k_tile) * (1.0 / math.sqrt(HEAD))
            top = jnp.max(logits, axis=-1, keepdims=True)
            expo = jnp.exp(logits - top)
            weight = (expo / jnp.sum(expo, axis=-1, keepdims=True)).astype(BF16)
            gathered = jnp.where(head_of == h, dot(weight, v_tile), gathered)
        outs.append(gathered.astype(BF16))
    self_proj = dot(jnp.concatenate(outs, axis=1), wo_self[...])
    after_self = layer_norm(after_cross.astype(F32) + self_proj, gain_self[...]).astype(BF16)
    halves = (slice(0, 96), slice(96, nq))

    def x_out(part, d):
        rows = halves[part]
        k = 2 * (d // 2) + part
        return send(mine_out.at[rows], around.at[d - 1, rows], s5.at[k], v5.at[k], x_peer(d))

    def x_pass(part):
        rows = halves[part]
        back, d = ((1, 1), (NX - 1, NX - 1))[part]
        return send(around.at[back - 1, rows], around.at[1, rows], s5.at[4 + part], v5.at[4 + part], x_peer(d))

    def finish(part, back):
        rows = halves[part]
        k = 2 * back + part
        i = core * NX + lax.rem(x - back + NX, NX)
        source = mine_out.at[rows] if back == 0 else around.at[back - 1, rows]
        return (
            pltpu.make_async_copy(source, out.at[i, rows], store_sem.at[k]),
            send(source, out.at[i, rows], s6.at[k], v6.at[k], partner),
        )

    def pass_on(part, back):
        for copy in finish(part, back)[::-1]:
            copy.start()

    for part in range(2):
        rows = halves[part]
        hidden = jnp.maximum(dot(after_self[rows], w_in[...]), 0.0).astype(BF16)
        ffn = dot(hidden, w_out[...])
        mine_out[rows] = layer_norm(after_self[rows].astype(F32) + ffn, gain_ffn[...]).astype(BF16)
        x_out(part, 1).start()
        x_out(part, NX - 1).start()
        pass_on(part, 0)
    x_out(0, 1).wait_recv()
    x_pass(0).start()
    pass_on(0, 1)
    x_out(0, NX - 1).wait_recv()
    pass_on(0, NX - 1)
    x_out(1, NX - 1).wait_recv()
    x_pass(1).start()
    pass_on(1, NX - 1)
    x_out(1, 1).wait_recv()
    pass_on(1, 1)
    x_pass(0).wait_recv()
    pass_on(0, 2)
    x_pass(1).wait_recv()
    pass_on(1, 2)
    for part in range(2):
        x_out(part, 1).wait_send()
        x_out(part, NX - 1).wait_send()
        x_pass(part).wait_send()
        for back in range(NX):
            for copy in finish(part, back):
                copy.wait()


def local(
    queries, query_pos, pixels, pixel_pos, masks, wq_cross, wk_cross, wv_cross, wo_cross, gain_cross, w_qkv, wo_self,
    gain_self, w_in, w_out, gain_ffn,
):
    images, nq, width = queries.shape
    pix = pixels.shape[1]
    dma = pltpu.SemaphoreType.DMA
    vmem = pltpu.VMEM
    operands = (
        queries, query_pos, pixels, pixel_pos, masks, wq_cross, wk_cross, wv_cross, wo_cross, gain_cross[None], w_qkv,
        wo_self, gain_self[None], w_in, w_out, gain_ffn[None],
    )
    scratch = [vmem(a.shape, a.dtype) for a in operands] + [
        dma((images, 3)),
        dma((5,)),
        dma((8,)),
        vmem((width, width), BF16),
        vmem((width, width), BF16),
        vmem((pix, pix), BF16),
        vmem((pix, width), BF16),
        vmem((HEADS, HEAD + 16, pix), BF16),
        vmem((width, LANES), BF16),
        vmem((pix + 8, LANES), F32),
        vmem((pix, width), BF16),
        vmem((HEADS, HEAD + 16, pix), BF16),
        vmem((width, LANES), BF16),
        vmem((pix + 8, LANES), F32),
        vmem((HEADS, pix, LANES), F32),
        vmem((HEADS, pix, LANES), BF16),
        vmem((width, LANES), F32),
        vmem((2 * HEADS, LANES), F32),
        vmem((NX, width, LANES), BF16),
        vmem((NX, 2 * HEADS, LANES), F32),
        vmem((NX, width, LANES), BF16),
        vmem((NX, 2 * HEADS, LANES), F32),
        vmem((NX, width, LANES), BF16),
        vmem((NX, 2 * HEADS, LANES), F32),
        vmem((NX - 1, width, LANES), BF16),
        vmem((NX - 1, 2 * HEADS, LANES), F32),
        vmem((NZ, HEAD, LANES), BF16),
        vmem((NZ, 8, 128), F32),
        vmem((NZ - 1, HEAD, LANES), BF16),
        vmem((NZ - 1, 8, 128), F32),
        vmem((NZ, HEAD, LANES), BF16),
        vmem((nq, width), BF16),
        vmem((NX - 1, nq, width), BF16),
        dma((NX, 2)),
        dma((NX, 2)),
        dma((NX - 1, 2)),
        dma((NX - 1, 2)),
        dma((NZ - 1, 2)),
        dma((NZ - 1, 2)),
        dma((NZ - 1,)),
        dma((NZ - 1,)),
        dma((6,)),
        dma((6,)),
        dma((2 * NX,)),
        dma((2 * NX,)),
        dma((2 * NX,)),
    ]
    return pl.pallas_call(
        kernel,
        out_shape=jax.ShapeDtypeStruct((images, nq, width), BF16),
        in_specs=[pl.BlockSpec(memory_space=pltpu.HBM)] * 16,
        out_specs=pl.BlockSpec(memory_space=pltpu.HBM),
        scratch_shapes=scratch,
        compiler_params=pltpu.CompilerParams(
            collective_id=0, has_side_effects=True, vmem_limit_bytes=67043328
        ),
        name="decoder_layer",
    )(*operands)


def solution(mesh):
    placed = (
        P("dp", None, None),
        P(),
        P("dp", "space", None),
        P("space", None),
        P("dp", None, "space"),
    ) + (P(),) * 11
    return jax.shard_map(local, mesh=mesh, in_specs=placed, out_specs=P("dp", None, None), check_vma=False)
```
